512 devices in a mesh: ops: 128 (over x, z_hi, y), grp: 4 (over z_lo, core).
Axes of the slice: x: 4, y: 8, z: 8 (z_hi: 4, z_lo: 2; z = z_hi * 2 + z_lo), core: 2. Of those that a mesh axis runs over, the one named last changes fastest.
Arguments:
- wave: bfloat16 [32, 512, 512], P(None, 'ops'), may hold values from -12 to 12
- diag_energy: float32 [32, 512, 512], P(None, 'ops'), may hold values from 0.5 to 2
- left_ops: bfloat16 [512, 512, 512], P(('ops', 'grp')), may hold values from -0.046875 to 0.046875
- right_ops: bfloat16 [512, 512, 512], P(('ops', 'grp')), may hold values from -0.25 to 0.25
- pair_sectors: int32 [512, 2], replicated, may hold values from 0 to 31, all different within a row
- sector_slot: int32 [32], replicated, may hold values from 0 to 31, each once
Outputs:
- residual: float32 [32, 512, 512], P(None, 'ops', 'grp')
- sigma_out: float32 [32, 512, 512], P(None, 'ops', 'grp')
The draws below stay inside these ranges and needn't reach their ends.
Inputs may be any that keep to these rules, and one draw needn't show every extreme that they name: `pair_sectors`: each row names two different sectors; every sector is named by some row. `sector_slot`: each slot once.
All inputs are finite; a program needn't handle non-finite values.
Results may differ from the reference program's by a relative error of at most 0.0062.
Values may be sent and summed in bfloat16 or wider, within the bound.
No kernel may reach another device: no remote copies, remote signals or barrier semaphores. Data moves between devices by JAX's collectives and lax.ppermute only.
A program may use at most 64 MiB of HBM per device.

```python
import math
import jax
import jax.numpy as jnp
from jax import lax

SECT = 32
BLK = 512
PAIRS = 512


def draw_wave(key, part):
    keys = jax.random.split(key, 1)
    base = jax.random.normal(keys[0], (SECT, BLK, BLK), jnp.float32)
    rows = jnp.arange(BLK, dtype=jnp.float32) / (BLK - 1)
    rising = jnp.sqrt(1.0 + 2.0 * rows)
    value = base * rising[None, :, None]
    return jnp.clip(value, -12.0, 12.0).astype(jnp.bfloat16)


def block_scale(rng, extent, shards, low, top_value):
    factor_of, own = 1.0, jax.random.fold_in(rng, 6)
    for axis_at, blocks in shards:
        steps = jnp.exp(jax.random.uniform(jax.random.fold_in(own, axis_at), (blocks,), jnp.float32, low / len(shards), top_value / len(shards)))
        factor_of = factor_of * jnp.repeat(steps, extent[axis_at] // blocks).reshape([-1 if axis == axis_at else 1 for axis in range(len(extent))])
    return factor_of


def choose_distinct(stream_key, rows, count, top, lift):
    sequence = jax.random.permutation(jax.random.fold_in(stream_key, 1), count)
    favour = sequence
    for power in range(3):
        favour = favour * favour // count
    favour = favour * lift // count
    chance = jax.random.randint(jax.random.fold_in(stream_key, 2), (rows, count), 0, 4096) + favour
    holders = jax.random.permutation(jax.random.fold_in(stream_key, 3), rows)[jnp.arange(count) % rows]
    chance = jnp.where(jnp.arange(rows)[:, None] == holders[None, :], 1 << 14, chance)
    merit = chance * count + jnp.arange(count)
    return lax.top_k(merit.astype(jnp.int32), top)[1].astype(jnp.int32)


def scatter_about(rng, extent, spread, bound, cuts=(), kind=jnp.bfloat16):
    entries = jax.random.normal(rng, extent, jnp.float32) * spread
    if len(cuts) > 0:
        entries = block_scale(rng, extent, cuts, -0.22, 0.18) * entries
    return jnp.clip(entries, min=-bound, max=bound).astype(kind)


def setup_inputs(seed: int = 0) -> dict:
    seeds = jax.random.split(jax.random.key(seed), 7)
    return {
        "wave": draw_wave(jax.random.fold_in(seeds[6], 71), 0),
        "diag_energy": jnp.clip(jnp.exp(math.log(2.0) - 1.3862944 * jax.random.uniform(seeds[1], (SECT, BLK, BLK), jnp.float32) ** block_scale(seeds[1], (SECT, BLK, BLK), ((1, 128),), -0.2, 0.2)), 0.5, 2.0),
        "left_ops": scatter_about(seeds[2], (PAIRS, BLK, BLK), (BLK * 2 * PAIRS // SECT) ** -0.5, 0.046875, ((0, 512),)),
        "right_ops": scatter_about(seeds[3], (PAIRS, BLK, BLK), BLK ** -0.5, 0.25, ((0, 512),)),
        "pair_sectors": choose_distinct(seeds[4], PAIRS, SECT, 2, 512),
        "sector_slot": jax.random.permutation(seeds[5], SECT).astype(jnp.int32),
    }


def apply_pairs(vector, diag_energy, left_ops, right_ops, source, target):
    running = diag_energy * vector.astype(jnp.float32)

    def visit(accum, payload):
        left_op, right_op, from_slot, to_slot = payload
        source_block = lax.dynamic_index_in_dim(vector, from_slot, 0, keepdims=False)
        target_block = lax.dynamic_index_in_dim(vector, to_slot, 0, keepdims=False)
        inner_half = jnp.dot(left_op, source_block, preferred_element_type=jnp.float32).astype(jnp.bfloat16)
        forward = jnp.dot(inner_half, right_op, preferred_element_type=jnp.float32)
        flipped = jnp.dot(left_op.T, target_block, preferred_element_type=jnp.float32).astype(jnp.bfloat16)
        adjoint = jnp.dot(flipped, right_op.T, preferred_element_type=jnp.float32)
        accum = accum.at[to_slot].add(forward)
        accum = accum.at[from_slot].add(adjoint)
        return accum, None

    return lax.scan(visit, running, (left_ops, right_ops, source, target))[0]


def reference(wave, diag_energy, left_ops, right_ops, pair_sectors, sector_slot):
    stored = jnp.take(sector_slot, pair_sectors, axis=0).astype(jnp.int32)
    source = stored[:, 0]
    target = stored[:, 1]
    applied = apply_pairs(wave, diag_energy, left_ops, right_ops, source, target)
    wave_wide = wave.astype(jnp.float32)
    rayleigh = jnp.sum(wave_wide * applied) / jnp.sum(wave_wide * wave_wide)
    residual = applied - rayleigh * wave_wide
    residual_half = residual.astype(jnp.bfloat16)
    sigma_out = apply_pairs(residual_half, diag_energy, left_ops, right_ops, source, target)
    return residual, sigma_out
```

```python
import functools

import jax
import jax.numpy as jnp
from jax import lax
from jax.experimental import pallas as pl
from jax.experimental.pallas import tpu as pltpu
from jax.sharding import Mesh
from jax.sharding import PartitionSpec as P

OPS = ("ops_0", "ops_1", "ops_2")
OPS_GRP = ("ops_0", "ops_1", "ops_2", "grp")
F32 = jnp.float32
BF16 = jnp.bfloat16
VMEM = pl.BlockSpec(memory_space=pltpu.VMEM)
CONTRACT_ROWS = (((0,), (0,)), ((), ()))
CONTRACT_COLUMNS = (((1,), (1,)), ((), ()))


def iota(shape, dim):
    return lax.broadcasted_iota(jnp.int32, shape, dim)


def one_hot(mask):
    return jnp.where(mask, 1.0, 0.0).astype(BF16)


def whole(value):
    return value.astype(F32).astype(BF16)


def select_kernel(groups, ends_ref, slot_ref, wave_ref, choose_ref, out_ref):
    grp = lax.axis_index("grp")
    pairs = ends_ref.shape[1]
    ops = pairs // groups
    sectors = slot_ref.shape[1]
    rows_here = wave_ref.shape[0] // sectors
    mine = one_hot(iota((pairs, ops), 0) == iota((pairs, ops), 1) * groups + grp)
    sector = jnp.dot(whole(ends_ref[...]), mine, preferred_element_type=F32)
    slot_row = whole(slot_ref[...])
    number = iota((sectors, ops), 0).astype(F32)
    message = iota((ops, 2 * ops * rows_here), 1)
    holder = iota((ops, 2 * ops * rows_here), 0)
    target = jnp.zeros((1, 2 * ops * rows_here), F32)
    for end in range(2):
        slot = jnp.dot(slot_row, one_hot(number == sector[end : end + 1]), preferred_element_type=F32)
        spread = one_hot(message // rows_here == holder * 2 + end)
        target += jnp.dot(slot.astype(BF16), spread, preferred_element_type=F32)
    row = (iota(target.shape, 1) % rows_here).astype(F32)
    wanted = target * rows_here + row
    choose = one_hot(iota(choose_ref.shape, 0).astype(F32) == wanted)
    choose_ref[...] = choose
    out_ref[...] = lax.dot_general(
        choose, wave_ref[...], CONTRACT_ROWS, preferred_element_type=F32
    ).astype(BF16)


def pair_kernel(fetched_ref, left_ref, right_ref, out_ref):
    block = left_ref.shape[0]
    width = right_ref.shape[0]
    tiles = block // 8
    fetched = fetched_ref[...].astype(F32).reshape(tiles, 2, 8, width)
    first, second = fetched[:, 0], fetched[:, 1]
    upper = lax.broadcasted_iota(jnp.int32, first.shape, 1) < 4
    source = jnp.where(upper, first, pltpu.roll(second, 4, 1)).reshape(block, width).astype(BF16)
    target = jnp.where(upper, pltpu.roll(first, 4, 1), second).reshape(block, width).astype(BF16)
    left, right = left_ref[...], right_ref[...]
    inner = jnp.dot(left, source, preferred_element_type=F32).astype(BF16)
    forward = jnp.dot(inner, right, preferred_element_type=F32).reshape(tiles, 8, width)
    flipped = lax.dot_general(left, target, CONTRACT_ROWS, preferred_element_type=F32).astype(BF16)
    adjoint = lax.dot_general(
        flipped, right, CONTRACT_COLUMNS, preferred_element_type=F32
    ).reshape(tiles, 8, width)
    first = jnp.where(upper, adjoint, pltpu.roll(forward, 4, 1))
    second = jnp.where(upper, pltpu.roll(adjoint, 4, 1), forward)
    out_ref[...] = jnp.stack((first, second), axis=1).reshape(2 * block, width).astype(BF16)


def limit(mib):
    return pltpu.CompilerParams(vmem_limit_bytes=mib << 20)


def select_rows(ends, slots, wave_rows, groups):
    ops = ends.shape[1] // groups
    messages = 2 * ops * (wave_rows.shape[0] // slots.shape[1])
    return pl.pallas_call(
        functools.partial(select_kernel, groups),
        out_shape=(
            jax.ShapeDtypeStruct((wave_rows.shape[0], messages), BF16),
            jax.ShapeDtypeStruct((messages, wave_rows.shape[1]), BF16),
        ),
        in_specs=[VMEM] * 3,
        out_specs=(VMEM, VMEM),
        compiler_params=limit(24),
        cost_estimate=pl.CostEstimate(flops=400_000_000, bytes_accessed=2 << 20, transcendentals=0),
    )(ends, slots, wave_rows)


def apply_pair(fetched, left, right):
    return pl.pallas_call(
        pair_kernel,
        out_shape=jax.ShapeDtypeStruct(fetched.shape, BF16),
        in_specs=[VMEM] * 3,
        out_specs=VMEM,
        compiler_params=limit(24),
        cost_estimate=pl.CostEstimate(flops=1_100_000_000, bytes_accessed=3 << 20, transcendentals=0),
    )(fetched, left, right)


def exchange(rows, ops_count):
    shaped = rows.reshape(ops_count, rows.shape[0] // ops_count, rows.shape[1])
    return lax.all_to_all(shaped, OPS, 0, 0, tiled=True).reshape(rows.shape)


def taken_together(value, axes):
    devices = lax.axis_size(axes)
    copies = jnp.broadcast_to(value[None], (devices, *value.shape))
    return jnp.sum(lax.all_to_all(copies, axes, 0, 0, tiled=True), axis=0)


def body(wave, diag_energy, left_ops, right_ops, pair_sectors, sector_slot):
    ops_count = lax.axis_size(OPS)
    grp_count = lax.axis_size("grp")
    sectors, rows_here, width = wave.shape
    rows = sectors * rows_here
    share = width // grp_count
    left, right = left_ops[0], right_ops[0]
    wave_rows = wave.reshape(rows, width)
    diag_rows = diag_energy.reshape(rows, width)
    choose, outgoing = select_rows(pair_sectors.T, sector_slot[None], wave_rows, grp_count)

    def partial_blocks(outgoing):
        fetched = exchange(outgoing, ops_count)
        arrived = exchange(apply_pair(fetched, left, right), ops_count)
        return jnp.dot(choose, arrived, preferred_element_type=F32)

    summed = partial_blocks(outgoing)
    summed = summed + lax.ppermute(summed, "grp", [(g, g ^ 1) for g in range(grp_count)])
    summed = summed + lax.ppermute(
        summed.astype(BF16), "grp", [(g, g ^ 2) for g in range(grp_count)]
    ).astype(F32)
    wave_wide = wave_rows.astype(F32)
    applied = diag_rows * wave_wide + summed
    products = jnp.stack((jnp.sum(wave_wide * applied), jnp.sum(wave_wide * wave_wide)))
    products = taken_together(taken_together(products, "ops_2"), ("ops_0", "ops_1"))
    residual = applied - (products[0] / products[1]) * wave_wide
    residual_half = residual.astype(BF16)
    outgoing = lax.dot_general(
        choose, residual_half, CONTRACT_ROWS, preferred_element_type=F32
    ).astype(BF16)
    summed = partial_blocks(outgoing)
    parts = summed.astype(BF16).reshape(rows, grp_count, share).transpose(1, 0, 2)
    parts = lax.all_to_all(parts, "grp", 0, 0, tiled=True)
    start = lax.axis_index("grp") * share

    def mine(value):
        return lax.dynamic_slice_in_dim(value, start, share, 1)

    sigma_out = mine(diag_rows) * mine(residual_half).astype(F32) + jnp.sum(
        parts.astype(F32), axis=0
    )
    shape = (sectors, rows_here, share)
    return mine(residual).reshape(shape), sigma_out.reshape(shape)


def solution(mesh):
    finer = Mesh(
        mesh.devices.reshape(4, 4, 8, mesh.shape["grp"]), ("ops_0", "ops_1", "ops_2", "grp")
    )
    return jax.shard_map(
        body,
        mesh=finer,
        in_specs=(
            P(None, OPS, None),
            P(None, OPS, None),
            P(OPS_GRP, None, None),
            P(OPS_GRP, None, None),
            P(),
            P(),
        ),
        out_specs=(P(None, OPS, "grp"), P(None, OPS, "grp")),
        check_vma=False,
    )
```

```python
import functools

import jax
import jax.numpy as jnp
from jax import lax
from jax.experimental import pallas as pl
from jax.experimental.pallas import tpu as pltpu
from jax.sharding import Mesh
from jax.sharding import PartitionSpec as P

OPS = ("ops_0", "ops_1", "ops_2")
OPS_GRP = ("ops_0", "ops_1", "ops_2", "grp")
F32 = jnp.float32
BF16 = jnp.bfloat16
VMEM = pl.BlockSpec(memory_space=pltpu.VMEM)
CONTRACT_ROWS = (((0,), (0,)), ((), ()))
CONTRACT_COLUMNS = (((1,), (1,)), ((), ()))
LANES = 128


def iota(shape, dim):
    return lax.broadcasted_iota(jnp.int32, shape, dim)


def one_hot(mask):
    return jnp.where(mask, 1.0, 0.0).astype(BF16)


def whole(value):
    return value.astype(F32).astype(BF16)


def dot(left, right):
    return jnp.dot(left, right, preferred_element_type=F32)


def in_three(value):
    high = value.astype(BF16).astype(F32)
    middle = (value - high).astype(BF16).astype(F32)
    low = (value - high - middle).astype(BF16).astype(F32)
    return high, middle, low


def total(value):
    return jnp.sum(jnp.sum(value, axis=0, keepdims=True), axis=1, keepdims=True)


def select_kernel(groups, ends_ref, slot_ref, wave_ref, choose_ref, every_ref, out_ref):
    grp = lax.axis_index("grp")
    pairs = ends_ref.shape[1]
    ops = pairs // groups
    sectors = slot_ref.shape[1]
    rows_here = wave_ref.shape[0] // sectors
    messages = 2 * ops * rows_here
    ends = ends_ref[...]
    slot_row = whole(slot_ref[...])
    number = iota((sectors, pairs), 0)
    mine = one_hot(iota((pairs, ops), 0) == iota((pairs, ops), 1) * groups + grp)
    message = iota((ops, messages), 1) // rows_here
    holder = iota((ops, messages), 0) * 2
    row = (iota((1, messages), 1) % rows_here).astype(F32)
    places = iota((choose_ref.shape[0], messages), 0).astype(F32)
    slots = [
        dot(slot_row, one_hot(number == ends[end : end + 1])).astype(BF16) for end in range(2)
    ]
    spreads = [one_hot(message == holder + end) for end in range(2)]

    def chosen(first, second):
        wanted = (dot(first, spreads[0]) + dot(second, spreads[1])) * rows_here + row
        return one_hot(places == wanted)

    choose = chosen(*(dot(slot, mine).astype(BF16) for slot in slots))
    choose_ref[...] = choose
    out_ref[...] = lax.dot_general(
        choose, wave_ref[...], CONTRACT_ROWS, preferred_element_type=F32
    ).astype(BF16)
    for part in range(groups):
        held = slice(part * ops, (part + 1) * ops)
        every_ref[:, part * messages : (part + 1) * messages] = chosen(
            slots[0][:, held], slots[1][:, held]
        )


def pair_products(fetched_ref, left_ref, right_ref):
    block = left_ref.shape[0]
    width = right_ref.shape[0]
    tiles = block // 8
    fetched = fetched_ref[...].astype(F32).reshape(tiles, 2, 8, width)
    even, odd = fetched[:, 0], fetched[:, 1]
    upper = lax.broadcasted_iota(jnp.int32, even.shape, 1) < 4
    source = jnp.where(upper, even, pltpu.roll(odd, 4, 1)).reshape(block, width).astype(BF16)
    target = jnp.where(upper, pltpu.roll(even, 4, 1), odd).reshape(block, width).astype(BF16)
    left, right = left_ref[...], right_ref[...]
    inner = dot(left, source).astype(BF16)
    forward = dot(inner, right).reshape(tiles, 8, width)
    flipped = lax.dot_general(left, target, CONTRACT_ROWS, preferred_element_type=F32).astype(BF16)
    adjoint = lax.dot_general(
        flipped, right, CONTRACT_COLUMNS, preferred_element_type=F32
    ).reshape(tiles, 8, width)
    return (
        (even, odd),
        (
            jnp.where(upper, adjoint, pltpu.roll(forward, 4, 1)),
            jnp.where(upper, pltpu.roll(adjoint, 4, 1), forward),
        ),
    )


def first_pair_kernel(fetched_ref, left_ref, right_ref, wave_ref, diag_ref, out_ref):
    (even, odd), (out_even, out_odd) = pair_products(fetched_ref, left_ref, right_ref)
    width = right_ref.shape[0]
    rows = out_ref.shape[0]
    out_ref[:, :width] = (
        jnp.stack((out_even, out_odd), axis=1).reshape(rows, width).astype(BF16)
    )
    wave = wave_ref[...].astype(F32)
    sums = (
        total(jnp.sum(even * out_even + odd * out_odd, axis=0)),
        total(diag_ref[...] * wave * wave),
        total(wave * wave),
    )
    lane = iota((1, LANES), 1)
    carried = jnp.zeros((1, LANES), F32)
    for at, term in enumerate(term for value in sums for term in in_three(value)):
        carried = jnp.where(lane == at, term, carried)
    out_ref[:, width:] = jnp.broadcast_to(carried, (rows, LANES)).astype(BF16)


def second_pair_kernel(fetched_ref, left_ref, right_ref, out_ref):
    _, (out_even, out_odd) = pair_products(fetched_ref, left_ref, right_ref)
    for part in range(out_ref.shape[2]):
        held = slice(part * LANES, (part + 1) * LANES)
        out_ref[:, 0, part] = out_even[:, :, held].astype(BF16)
        out_ref[:, 1, part] = out_odd[:, :, held].astype(BF16)


def gather_kernel(choose_ref, arrived_ref, out_ref):
    rows = choose_ref.shape[0]
    width = out_ref.shape[1]
    out_ref[:rows, :] = dot(choose_ref[...], arrived_ref[:, :width])
    carried = jnp.sum(arrived_ref[:, width:].astype(F32), axis=0, keepdims=True) * 0.125
    out_ref[rows:, :] = jnp.zeros((8, width), F32)
    out_ref[rows:, :LANES] = jnp.broadcast_to(carried, (8, LANES))


def add_kernel(rows, own_ref, other_ref, sum_ref, half_ref):
    summed = own_ref[...] + other_ref[...]
    sum_ref[...] = summed
    half_ref[:rows, :] = summed[:rows].astype(BF16)
    high, middle, low = in_three(summed[rows:])
    place = iota(high.shape, 0)
    terms = jnp.where(place == 0, high, jnp.where(place == 1, middle, low))
    half_ref[rows:, :] = jnp.where(place < 3, terms, 0.0).astype(BF16)


def residual_kernel(
    groups, own_ref, other_ref, wave_ref, diag_ref, choose_ref, residual_ref, base_ref, out_ref
):
    grp = lax.axis_index("grp")
    rows = wave_ref.shape[0]
    share = residual_ref.shape[1]
    carried = own_ref[rows : rows + 1, :] + jnp.sum(
        other_ref[rows:, :].astype(F32), axis=0, keepdims=True
    )
    lane = iota(carried.shape, 1)
    pairs_part = total(jnp.where(lane < 3, carried, 0.0))
    diag_part = total(jnp.where((lane >= 3) & (lane < 6), carried, 0.0)) / groups
    square = total(jnp.where((lane >= 6) & (lane < 9), carried, 0.0)) / groups
    rayleigh = (pairs_part + diag_part) / square
    wave = wave_ref[...].astype(F32)
    applied = diag_ref[...] * wave + (own_ref[:rows, :] + other_ref[:rows, :].astype(F32))
    residual = applied - rayleigh * wave
    half = residual.astype(BF16)
    base = diag_ref[...] * half.astype(F32)
    for part in range(groups):

        @pl.when(grp == part)
        def _():
            residual_ref[...] = residual[:, part * share : (part + 1) * share]
            base_ref[...] = base[:, part * share : (part + 1) * share]

    out_ref[...] = lax.dot_general(
        choose_ref[...], half, CONTRACT_ROWS, preferred_element_type=F32
    ).astype(BF16)


def final_kernel(every_ref, arrived_ref, base_ref, out_ref):
    out_ref[...] = base_ref[...] + dot(every_ref[...], arrived_ref[...])


def call(kernel, outs, flops, *args):
    specs = jax.tree.map(lambda _: VMEM, outs)
    size = sum(arg.size * arg.dtype.itemsize for arg in args)
    return pl.pallas_call(
        kernel,
        out_shape=outs,
        in_specs=[VMEM] * len(args),
        out_specs=specs,
        compiler_params=pltpu.CompilerParams(vmem_limit_bytes=24 << 20),
        cost_estimate=pl.CostEstimate(flops=flops, bytes_accessed=2 * size, transcendentals=0),
    )(*args)


def array(shape, dtype):
    return jax.ShapeDtypeStruct(shape, dtype)


def exchange(value, axes):
    devices = lax.axis_size(axes)
    shaped = value.reshape(devices, -1, value.shape[-1])
    return lax.all_to_all(shaped, axes, 0, 0, tiled=True).reshape(-1, value.shape[-1])


def body(wave, diag_energy, left_ops, right_ops, pair_sectors, sector_slot):
    ops = lax.axis_size(OPS)
    groups = lax.axis_size("grp")
    sectors, rows_here, width = wave.shape
    rows = sectors * rows_here
    share = width // groups
    messages = 2 * ops * rows_here
    left, right = left_ops[0], right_ops[0]
    wave = wave.reshape(rows, width)
    diag = diag_energy.reshape(rows, width)
    choose, every, outgoing = call(
        functools.partial(select_kernel, groups),
        (
            array((rows, messages), BF16),
            array((rows, groups * messages), BF16),
            array((messages, width), BF16),
        ),
        400_000_000,
        pair_sectors.T,
        sector_slot[None],
        wave,
    )
    fetched = exchange(outgoing, OPS)
    blocks = call(
        first_pair_kernel,
        array((messages, width + LANES), BF16),
        1_100_000_000,
        fetched,
        left,
        right,
        wave,
        diag,
    )
    arrived = exchange(blocks, OPS)
    own = call(gather_kernel, array((rows + 8, width), F32), 150_000_000, choose, arrived)
    other = lax.ppermute(own, "grp", [(g, g ^ 1) for g in range(groups)])
    own, half = call(
        functools.partial(add_kernel, rows),
        (array(own.shape, F32), array(own.shape, BF16)),
        1_000_000,
        own,
        other,
    )
    other = lax.ppermute(half, "grp", [(g, g ^ 2) for g in range(groups)])
    residual, base, outgoing = call(
        functools.partial(residual_kernel, groups),
        (
            array((rows, share), F32),
            array((rows, share), F32),
            array((messages, width), BF16),
        ),
        150_000_000,
        own,
        other,
        wave,
        diag,
        choose,
    )
    fetched = exchange(outgoing, OPS)
    blocks = call(
        second_pair_kernel,
        array((ops // 2, 2, groups, 2 * rows_here, share), BF16),
        1_100_000_000,
        fetched,
        left,
        right,
    )
    arrived = exchange(blocks, OPS_GRP)
    sigma_out = call(final_kernel, array((rows, share), F32), 150_000_000, every, arrived, base)
    shape = (sectors, rows_here, share)
    return residual.reshape(shape), sigma_out.reshape(shape)


def solution(mesh):
    finer = Mesh(
        mesh.devices.reshape(4, 4, 8, mesh.shape["grp"]), ("ops_0", "ops_1", "ops_2", "grp")
    )
    return jax.shard_map(
        body,
        mesh=finer,
        in_specs=(
            P(None, OPS, None),
            P(None, OPS, None),
            P(OPS_GRP, None, None),
            P(OPS_GRP, None, None),
            P(),
            P(),
        ),
        out_specs=(P(None, OPS, "grp"), P(None, OPS, "grp")),
        check_vma=False,
    )
```

```python
import functools

import jax
import jax.numpy as jnp
from jax import lax
from jax.experimental import pallas as pl
from jax.experimental.pallas import tpu as pltpu
from jax.sharding import Mesh
from jax.sharding import PartitionSpec as P

OPS = ("ops_0", "ops_1", "ops_2", "ops_3")
OPS_GRP = (*OPS, "grp")
NEAR = ("ops_0", "ops_3", "grp")
FAR = ("ops_1", "ops_2")
F32 = jnp.float32
BF16 = jnp.bfloat16
VMEM = pl.BlockSpec(memory_space=pltpu.VMEM)
CONTRACT_ROWS = (((0,), (0,)), ((), ()))
CONTRACT_COLUMNS = (((1,), (1,)), ((), ()))


def iota(shape, dim):
    return lax.broadcasted_iota(jnp.int32, shape, dim)


def one_hot(mask):
    return jnp.where(mask, 1.0, 0.0).astype(BF16)


def whole(value):
    return value.astype(F32).astype(BF16)


def dot(left, right):
    return jnp.dot(left, right, preferred_element_type=F32)


def in_three(value):
    high = value.astype(BF16).astype(F32)
    middle = (value - high).astype(BF16).astype(F32)
    low = (value - high - middle).astype(BF16).astype(F32)
    return high, middle, low


def total(value):
    return jnp.sum(jnp.sum(value, axis=0, keepdims=True), axis=1, keepdims=True)


def select_kernel(
    groups, inner, ends_ref, slot_ref, wave_ref, near_ref, every_ref, out_ref
):
    grp = lax.axis_index("grp")
    far = lax.axis_index("ops_1") * lax.axis_size("ops_2") + lax.axis_index("ops_2")
    far_count = lax.axis_size("ops_1") * lax.axis_size("ops_2")
    pairs = ends_ref.shape[1]
    ops = pairs // groups
    sectors = slot_ref.shape[1]
    rows = wave_ref.shape[0]
    rows_here = rows // sectors
    ends = ends_ref[...]
    slot_row = whole(slot_ref[...])
    number = iota((sectors, pairs), 0)
    slots = [
        dot(slot_row, one_hot(number == ends[end : end + 1])).astype(BF16) for end in range(2)
    ]

    def spreads_of(count):
        shape = (count, 2 * count * rows_here)
        message = iota(shape, 1) // rows_here
        return [one_hot(message == iota(shape, 0) * 2 + end) for end in range(2)]

    def chosen(slots, spreads):
        messages = spreads[0].shape[1]
        row = (iota((1, messages), 1) % rows_here).astype(F32)
        wanted = sum(dot(slot, spread) for slot, spread in zip(slots, spreads)) * rows_here + row
        return one_hot(iota((rows, messages), 0).astype(F32) == wanted)

    spreads = spreads_of(ops)
    mine = one_hot(iota((pairs, ops), 0) == iota((pairs, ops), 1) * groups + grp)
    choose = chosen([dot(slot, mine).astype(BF16) for slot in slots], spreads)
    out_ref[...] = lax.dot_general(
        choose, wave_ref[...], CONTRACT_ROWS, preferred_element_type=F32
    ).astype(BF16)
    messages = choose.shape[1]
    for part in range(groups):
        held = slice(part * ops, (part + 1) * ops)
        every_ref[:, part * messages : (part + 1) * messages] = chosen(
            [slot[:, held] for slot in slots], spreads
        )
    near_count = pairs // far_count
    member = iota((pairs, near_count), 1)
    pair = (member // inner * far_count + far) * inner + member % inner
    near = one_hot(iota((pairs, near_count), 0) == pair)
    near_ref[...] = chosen(
        [dot(slot, near).astype(BF16) for slot in slots], spreads_of(near_count)
    )


def pair_products(even, odd, left_ref, right_ref, right_copy):
    block = left_ref.shape[0]
    tiles, _, width = even.shape
    upper = lax.broadcasted_iota(jnp.int32, even.shape, 1) < 4
    source = jnp.where(upper, even, pltpu.roll(odd, 4, 1)).reshape(block, width).astype(BF16)
    target = jnp.where(upper, pltpu.roll(even, 4, 1), odd).reshape(block, width).astype(BF16)
    left = left_ref[...]
    inner = dot(left, source).astype(BF16)
    flipped = lax.dot_general(left, target, CONTRACT_ROWS, preferred_element_type=F32).astype(BF16)
    right_copy.wait()
    right = right_ref[...]
    forward = dot(inner, right).reshape(tiles, 8, width)
    adjoint = lax.dot_general(
        flipped, right, CONTRACT_COLUMNS, preferred_element_type=F32
    ).reshape(tiles, 8, width)
    return (
        jnp.where(upper, adjoint, pltpu.roll(forward, 4, 1)),
        jnp.where(upper, pltpu.roll(adjoint, 4, 1), forward),
    )


def first_pair_kernel(
    fetched_ref, left_ref, right_hbm, wave_ref, diag_ref, out_ref, right_ref, done
):
    copy = pltpu.make_async_copy(right_hbm, right_ref, done)
    copy.start()
    width = right_ref.shape[0]
    tiles = left_ref.shape[0] // 8
    blocks, _, groups, slots, _, share = out_ref.shape
    far = slots - 1
    fetched = fetched_ref[...].astype(F32).reshape(tiles, 2, 8, width)
    even, odd = fetched[:, 0], fetched[:, 1]
    products = pair_products(even, odd, left_ref, right_ref, copy)
    for block in range(blocks):
        for parity, product in enumerate(products):
            for grp in range(groups):
                out_ref[block, parity, grp, :far] = product[
                    block * far : (block + 1) * far, :, grp * share : (grp + 1) * share
                ].astype(BF16)
    wave = wave_ref[...].astype(F32)
    sums = (
        total(jnp.sum(even * products[0] + odd * products[1], axis=0)),
        total(diag_ref[...] * wave * wave),
        total(wave * wave),
    )
    lane = iota((1, share), 1)
    carried = jnp.zeros((1, share), F32)
    for at, term in enumerate(term for value in sums for term in in_three(value)):
        carried = jnp.where(lane == at, term, carried)
    carried = jnp.broadcast_to(carried, (8, share)).astype(BF16)
    for block in range(blocks):
        for parity in range(2):
            for grp in range(groups):
                out_ref[block, parity, grp, far] = carried


def second_pair_kernel(fetched_ref, left_ref, right_hbm, out_ref, right_ref, done):
    copy = pltpu.make_async_copy(right_hbm, right_ref, done)
    copy.start()
    groups, share = fetched_ref.shape[2], fetched_ref.shape[4]
    even, odd = (
        jnp.concatenate(
            [fetched_ref[:, parity, grp].astype(F32) for grp in range(groups)], axis=2
        )
        for parity in range(2)
    )
    products = pair_products(even, odd, left_ref, right_ref, copy)
    for parity, product in enumerate(products):
        for grp in range(groups):
            out_ref[:, parity, grp] = product[:, :, grp * share : (grp + 1) * share].astype(BF16)


def gather_kernel(near_ref, arrived_ref, out_ref):
    members, slots, _, share = arrived_ref.shape
    far = slots - 1
    rows = near_ref.shape[0]
    near = near_ref[...]
    carried = jnp.sum(arrived_ref[:, far].astype(F32), axis=0)
    high, middle, low = in_three(carried)
    place = iota(carried.shape, 0)
    terms = jnp.where(place == 0, high, jnp.where(place == 1, middle, low))
    terms = jnp.where(place < 3, terms, 0.0).astype(BF16)
    for at in range(far):
        arrived = arrived_ref[:, at].reshape(members * 8, share)
        out_ref[at, :rows] = dot(near, arrived).astype(BF16)
        out_ref[at, rows:] = terms


def residual_kernel(groups, arrived_ref, wave_ref, diag_ref, every_ref, residual_ref, base_ref, out_ref):
    rows, share = residual_ref.shape
    arrived = jnp.sum(arrived_ref[...].astype(F32), axis=0)
    carried = jnp.sum(arrived[rows:], axis=0, keepdims=True)
    lane = iota(carried.shape, 1)
    pairs_part = total(jnp.where(lane < 3, carried, 0.0))
    diag_part = total(jnp.where((lane >= 3) & (lane < 6), carried, 0.0)) / groups
    square = total(jnp.where((lane >= 6) & (lane < 9), carried, 0.0)) / groups
    rayleigh = (pairs_part + diag_part) / square
    mine = pl.ds(pl.multiple_of(lax.axis_index("grp") * share, share), share)
    wave = wave_ref[:, mine].astype(F32)
    diag = diag_ref[:, mine]
    residual = diag * wave + arrived[:rows] - rayleigh * wave
    half = residual.astype(BF16)
    residual_ref[...] = residual
    base_ref[...] = diag * half.astype(F32)
    out_ref[...] = lax.dot_general(
        every_ref[...], half, CONTRACT_ROWS, preferred_element_type=F32
    ).astype(BF16)


def final_kernel(every_ref, arrived_ref, base_ref, out_ref):
    out_ref[...] = base_ref[...] + dot(every_ref[...], arrived_ref[...])


def call(kernel, outs, flops, *args, scratch=(), far_away=()):
    specs = jax.tree.map(lambda _: VMEM, outs)
    size = sum(arg.size * arg.dtype.itemsize for arg in args)
    return pl.pallas_call(
        kernel,
        out_shape=outs,
        in_specs=[
            pl.BlockSpec(memory_space=pltpu.HBM) if at in far_away else VMEM
            for at in range(len(args))
        ],
        out_specs=specs,
        scratch_shapes=scratch,
        compiler_params=pltpu.CompilerParams(vmem_limit_bytes=24 << 20),
        cost_estimate=pl.CostEstimate(flops=flops, bytes_accessed=2 * size, transcendentals=0),
    )(*args)


def array(shape, dtype):
    return jax.ShapeDtypeStruct(shape, dtype)


def exchange(value, axes):
    return lax.all_to_all(value, axes, 0, 0, tiled=True)


def body(wave, diag_energy, left_ops, right_ops, pair_sectors, sector_slot):
    ops = lax.axis_size(OPS)
    groups = lax.axis_size("grp")
    far = lax.axis_size(FAR)
    near = lax.axis_size(NEAR)
    blocks = lax.axis_size("ops_0")
    sectors, rows_here, width = wave.shape
    rows = sectors * rows_here
    share = width // groups
    messages = 2 * ops * rows_here
    left, right = left_ops[0], right_ops[0]
    wave = wave.reshape(rows, width)
    diag = diag_energy.reshape(rows, width)
    held = (pltpu.VMEM(right.shape, BF16), pltpu.SemaphoreType.DMA)
    near_choose, every, outgoing = call(
        functools.partial(select_kernel, groups, near // blocks),
        (
            array((rows, 2 * near * rows_here), BF16),
            array((rows, groups * messages), BF16),
            array((messages, width), BF16),
        ),
        400_000_000,
        pair_sectors.T,
        sector_slot[None],
        wave,
    )
    fetched = exchange(outgoing.reshape(ops, -1, width), OPS).reshape(messages, width)
    scattered = call(
        first_pair_kernel,
        array((blocks, 2, groups, far + 1, 8, share), BF16),
        1_100_000_000,
        fetched,
        left,
        right,
        wave,
        diag,
        scratch=held,
        far_away=(2,),
    )
    arrived = exchange(scattered.reshape(near, far + 1, 8, share), NEAR)
    partial = call(
        gather_kernel, array((far, rows + 8, share), BF16), 150_000_000, near_choose, arrived
    )
    arrived = exchange(partial, FAR)
    residual, base, outgoing = call(
        functools.partial(residual_kernel, groups),
        (
            array((rows, share), F32),
            array((rows, share), F32),
            array((groups * messages, share), BF16),
        ),
        150_000_000,
        arrived,
        wave,
        diag,
        every,
    )
    fetched = exchange(outgoing.reshape(ops * groups, -1, share), OPS_GRP)
    shape = (ops // 2, 2, groups, 2 * rows_here, share)
    scattered = call(
        second_pair_kernel,
        array(shape, BF16),
        1_100_000_000,
        fetched.reshape(shape),
        left,
        right,
        scratch=held,
        far_away=(2,),
    )
    arrived = exchange(scattered.reshape(ops * groups, -1, share), OPS_GRP)
    sigma_out = call(
        final_kernel,
        array((rows, share), F32),
        150_000_000,
        every,
        arrived.reshape(groups * messages, share),
        base,
    )
    shape = (sectors, rows_here, share)
    return residual.reshape(shape), sigma_out.reshape(shape)


def solution(mesh):
    finer = Mesh(mesh.devices.reshape(4, 4, 4, 2, mesh.shape["grp"]), OPS_GRP)
    return jax.shard_map(
        body,
        mesh=finer,
        in_specs=(
            P(None, OPS, None),
            P(None, OPS, None),
            P(OPS_GRP, None, None),
            P(OPS_GRP, None, None),
            P(),
            P(),
        ),
        out_specs=(P(None, OPS, "grp"), P(None, OPS, "grp")),
        check_vma=False,
    )
```

```python
import functools

import jax
import jax.numpy as jnp
from jax import lax
from jax.experimental import pallas as pl
from jax.experimental.pallas import tpu as pltpu
from jax.sharding import Mesh
from jax.sharding import PartitionSpec as P

OPS = ("ops_0", "ops_1", "ops_2", "ops_3")
OPS_GRP = (*OPS, "grp")
NEAR = ("ops_0", "ops_3", "grp")
FAR = ("ops_1", "ops_2")
F32 = jnp.float32
BF16 = jnp.bfloat16
VMEM = pl.BlockSpec(memory_space=pltpu.VMEM)
CONTRACT_ROWS = (((0,), (0,)), ((), ()))
CONTRACT_COLUMNS = (((1,), (1,)), ((), ()))


def iota(shape, dim):
    return lax.broadcasted_iota(jnp.int32, shape, dim)


def one_hot(mask):
    return jnp.where(mask, 1.0, 0.0).astype(BF16)


def whole(value):
    return value.astype(F32).astype(BF16)


def dot(left, right):
    return jnp.dot(left, right, preferred_element_type=F32)


def in_three(value):
    high = value.astype(BF16).astype(F32)
    middle = (value - high).astype(BF16).astype(F32)
    low = (value - high - middle).astype(BF16).astype(F32)
    return high, middle, low


def total(value):
    return jnp.sum(jnp.sum(value, axis=0, keepdims=True), axis=1, keepdims=True)


def spreads_of(count, rows_here):
    shape = (count, 2 * count * rows_here)
    message = iota(shape, 1) // rows_here
    return [one_hot(message == iota(shape, 0) * 2 + end) for end in range(2)]


def chosen(slots, spreads, rows, rows_here):
    messages = spreads[0].shape[1]
    row = (iota((1, messages), 1) % rows_here).astype(F32)
    wanted = sum(dot(slot, spread) for slot, spread in zip(slots, spreads)) * rows_here + row
    return one_hot(iota((rows, messages), 0).astype(F32) == wanted)


def slots_of(ends_ref, slot_ref):
    ends = ends_ref[...]
    slot_row = whole(slot_ref[...])
    number = iota((slot_row.shape[1], ends.shape[1]), 0)
    return [
        dot(slot_row, one_hot(number == ends[end : end + 1])).astype(BF16) for end in range(2)
    ]


def select_kernel(groups, ends_ref, slot_ref, wave_ref, out_ref):
    grp = lax.axis_index("grp")
    pairs = ends_ref.shape[1]
    ops = pairs // groups
    sectors, rows_here, width = wave_ref.shape
    rows = sectors * rows_here
    mine = one_hot(iota((pairs, ops), 0) == iota((pairs, ops), 1) * groups + grp)
    slots = [dot(slot, mine).astype(BF16) for slot in slots_of(ends_ref, slot_ref)]
    choose = chosen(slots, spreads_of(ops, rows_here), rows, rows_here)
    wave = wave_ref[...].astype(F32).reshape(rows, width).astype(BF16)
    out_ref[...] = lax.dot_general(
        choose, wave, CONTRACT_ROWS, preferred_element_type=F32
    ).astype(BF16)


def table_kernel(groups, inner, ends_ref, slot_ref, near_ref, every_ref):
    far = lax.axis_index("ops_1") * lax.axis_size("ops_2") + lax.axis_index("ops_2")
    far_count = lax.axis_size("ops_1") * lax.axis_size("ops_2")
    pairs = ends_ref.shape[1]
    ops = pairs // groups
    rows = near_ref.shape[0]
    rows_here = rows // slot_ref.shape[1]
    slots = slots_of(ends_ref, slot_ref)
    spreads = spreads_of(ops, rows_here)
    messages = 2 * ops * rows_here
    for part in range(groups):
        held = slice(part * ops, (part + 1) * ops)
        every_ref[:, part * messages : (part + 1) * messages] = chosen(
            [slot[:, held] for slot in slots], spreads, rows, rows_here
        )
    near_count = pairs // far_count
    member = iota((pairs, near_count), 1)
    pair = (member // inner * far_count + far) * inner + member % inner
    near = one_hot(iota((pairs, near_count), 0) == pair)
    near_ref[...] = chosen(
        [dot(slot, near).astype(BF16) for slot in slots],
        spreads_of(near_count, rows_here),
        rows,
        rows_here,
    )


def pair_products(even, odd, left_ref, right_ref):
    block = left_ref.shape[0]
    tiles, _, width = even.shape
    upper = lax.broadcasted_iota(jnp.int32, even.shape, 1) < 4
    source = jnp.where(upper, even, pltpu.roll(odd, 4, 1)).reshape(block, width).astype(BF16)
    target = jnp.where(upper, pltpu.roll(even, 4, 1), odd).reshape(block, width).astype(BF16)
    left = left_ref[...]
    inner = dot(left, source).astype(BF16)
    flipped = lax.dot_general(left, target, CONTRACT_ROWS, preferred_element_type=F32).astype(BF16)
    right = right_ref[...]
    forward = dot(inner, right).reshape(tiles, 8, width)
    adjoint = lax.dot_general(
        flipped, right, CONTRACT_COLUMNS, preferred_element_type=F32
    ).reshape(tiles, 8, width)
    return (
        jnp.where(upper, adjoint, pltpu.roll(forward, 4, 1)),
        jnp.where(upper, pltpu.roll(adjoint, 4, 1), forward),
    )


def first_pair_kernel(
    fetched_ref, left_ref, right_ref, wave_ref, diag_ref, near_ref, out_ref
):
    width = right_ref.shape[0]
    tiles = left_ref.shape[0] // 8
    blocks, _, groups, slots, _, share = out_ref.shape
    far = slots - 1
    fetched = fetched_ref[...].astype(F32).reshape(tiles, 2, 8, width)
    even, odd = fetched[:, 0], fetched[:, 1]
    products = pair_products(even, odd, left_ref, right_ref)
    for block in range(blocks):
        for parity, product in enumerate(products):
            for grp in range(groups):
                out_ref[block, parity, grp, :far] = product[
                    block * far : (block + 1) * far, :, grp * share : (grp + 1) * share
                ].astype(BF16)
    wave = wave_ref[...].astype(F32)
    sums = (
        total(jnp.sum(even * products[0] + odd * products[1], axis=0)),
        total(diag_ref[...] * wave * wave),
        total(wave * wave),
    )
    lane = iota((1, share), 1)
    carried = jnp.zeros((1, share), F32)
    for at, term in enumerate(term for value in sums for term in in_three(value)):
        carried = jnp.where(lane == at, term, carried)
    carried = jnp.broadcast_to(carried, (8, share)).astype(BF16)
    for block in range(blocks):
        for parity in range(2):
            for grp in range(groups):
                out_ref[block, parity, grp, far] = carried


def second_pair_kernel(fetched_ref, left_ref, right_ref, out_ref):
    groups, share = fetched_ref.shape[2], fetched_ref.shape[4]
    even, odd = (
        jnp.concatenate(
            [fetched_ref[:, parity, grp].astype(F32) for grp in range(groups)], axis=2
        )
        for parity in range(2)
    )
    products = pair_products(even, odd, left_ref, right_ref)
    for parity, product in enumerate(products):
        for grp in range(groups):
            out_ref[:, parity, grp] = product[:, :, grp * share : (grp + 1) * share].astype(BF16)


def gather_kernel(near_ref, arrived_ref, out_ref):
    members, slots, _, share = arrived_ref.shape
    far = slots - 1
    rows = near_ref.shape[0]
    near = near_ref[...]
    carried = jnp.sum(arrived_ref[:, far].astype(F32), axis=0)
    high, middle, low = in_three(carried)
    place = iota(carried.shape, 0)
    terms = jnp.where(place == 0, high, jnp.where(place == 1, middle, low))
    terms = jnp.where(place < 3, terms, 0.0).astype(BF16)
    for at in range(far):
        arrived = arrived_ref[:, at].reshape(members * 8, share)
        out_ref[at, :rows] = dot(near, arrived).astype(BF16)
        out_ref[at, rows:] = terms


def residual_kernel(groups, arrived_ref, wave_ref, diag_ref, every_ref, residual_ref, base_ref, out_ref):
    rows, share = residual_ref.shape
    arrived = jnp.sum(arrived_ref[...].astype(F32), axis=0)
    carried = jnp.sum(arrived[rows:], axis=0, keepdims=True)
    lane = iota(carried.shape, 1)
    pairs_part = total(jnp.where(lane < 3, carried, 0.0))
    diag_part = total(jnp.where((lane >= 3) & (lane < 6), carried, 0.0)) / groups
    square = total(jnp.where((lane >= 6) & (lane < 9), carried, 0.0)) / groups
    rayleigh = (pairs_part + diag_part) / square
    mine = pl.ds(pl.multiple_of(lax.axis_index("grp") * share, share), share)
    wave = wave_ref[:, mine].astype(F32)
    diag = diag_ref[:, mine]
    residual = diag * wave + arrived[:rows] - rayleigh * wave
    half = residual.astype(BF16)
    residual_ref[...] = residual
    base_ref[...] = diag * half.astype(F32)
    out_ref[...] = lax.dot_general(
        every_ref[...], half, CONTRACT_ROWS, preferred_element_type=F32
    ).astype(BF16)


def final_kernel(every_ref, arrived_ref, base_ref, out_ref):
    out_ref[...] = base_ref[...] + dot(every_ref[...], arrived_ref[...])


def call(kernel, outs, flops, *args, grant=24):
    specs = jax.tree.map(lambda _: VMEM, outs)
    size = sum(arg.size * arg.dtype.itemsize for arg in args)
    return pl.pallas_call(
        kernel,
        out_shape=outs,
        in_specs=[VMEM] * len(args),
        out_specs=specs,
        compiler_params=pltpu.CompilerParams(vmem_limit_bytes=grant << 20),
        cost_estimate=pl.CostEstimate(flops=flops, bytes_accessed=2 * size, transcendentals=0),
    )(*args)


def array(shape, dtype):
    return jax.ShapeDtypeStruct(shape, dtype)


def exchange(value, axes):
    return lax.all_to_all(value, axes, 0, 0, tiled=True)


def body(wave, diag_energy, left_ops, right_ops, pair_sectors, sector_slot):
    ops = lax.axis_size(OPS)
    groups = lax.axis_size("grp")
    far = lax.axis_size(FAR)
    near = lax.axis_size(NEAR)
    blocks = lax.axis_size("ops_0")
    sectors, rows_here, width = wave.shape
    rows = sectors * rows_here
    share = width // groups
    messages = 2 * ops * rows_here
    left, right = left_ops[0], right_ops[0]
    pairs, slots = pair_sectors.T, sector_slot[None]
    outgoing = call(
        functools.partial(select_kernel, groups),
        array((messages, width), BF16),
        200_000_000,
        pairs,
        slots,
        wave,
        grant=60,
    )
    near_choose, every = call(
        functools.partial(table_kernel, groups, near // blocks),
        (
            array((rows, 2 * near * rows_here), BF16),
            array((rows, groups * messages), BF16),
        ),
        2_000_000_000,
        pairs,
        slots,
    )
    wave = wave.reshape(rows, width)
    diag = diag_energy.reshape(rows, width)
    fetched = exchange(outgoing.reshape(ops, -1, width), OPS).reshape(messages, width)
    scattered = call(
        first_pair_kernel,
        array((blocks, 2, groups, far + 1, 8, share), BF16),
        1_100_000_000,
        fetched,
        left,
        right,
        wave,
        diag,
        near_choose,
    )
    arrived = exchange(scattered.reshape(near, far + 1, 8, share), NEAR)
    partial = call(
        gather_kernel, array((far, rows + 8, share), BF16), 150_000_000, near_choose, arrived
    )
    arrived = exchange(partial, FAR)
    residual, base, outgoing = call(
        functools.partial(residual_kernel, groups),
        (
            array((rows, share), F32),
            array((rows, share), F32),
            array((groups * messages, share), BF16),
        ),
        150_000_000,
        arrived,
        wave,
        diag,
        every,
    )
    fetched = exchange(outgoing.reshape(ops * groups, -1, share), OPS_GRP)
    shape = (ops // 2, 2, groups, 2 * rows_here, share)
    scattered = call(
        second_pair_kernel,
        array(shape, BF16),
        1_100_000_000,
        fetched.reshape(shape),
        left,
        right,
    )
    arrived = exchange(scattered.reshape(ops * groups, -1, share), OPS_GRP)
    sigma_out = call(
        final_kernel,
        array((rows, share), F32),
        150_000_000,
        every,
        arrived.reshape(groups * messages, share),
        base,
    )
    shape = (sectors, rows_here, share)
    return residual.reshape(shape), sigma_out.reshape(shape)


def solution(mesh):
    finer = Mesh(mesh.devices.reshape(4, 4, 4, 2, mesh.shape["grp"]), OPS_GRP)
    return jax.shard_map(
        body,
        mesh=finer,
        in_specs=(
            P(None, OPS, None),
            P(None, OPS, None),
            P(OPS_GRP, None, None),
            P(OPS_GRP, None, None),
            P(),
            P(),
        ),
        out_specs=(P(None, OPS, "grp"), P(None, OPS, "grp")),
        check_vma=False,
    )
```

```python
import functools

import jax
import jax.numpy as jnp
from jax import lax
from jax.experimental import pallas as pl
from jax.experimental.pallas import tpu as pltpu
from jax.sharding import Mesh
from jax.sharding import PartitionSpec as P

OPS = ("ops_0", "ops_1", "ops_2", "ops_3")
OPS_GRP = (*OPS, "grp")
NEAR = ("ops_0", "ops_3", "grp")
FAR = ("ops_1", "ops_2")
F32 = jnp.float32
BF16 = jnp.bfloat16
VMEM = pl.BlockSpec(memory_space=pltpu.VMEM)
CONTRACT_ROWS = (((0,), (0,)), ((), ()))
CONTRACT_COLUMNS = (((1,), (1,)), ((), ()))


def iota(shape, dim):
    return lax.broadcasted_iota(jnp.int32, shape, dim)


def one_hot(mask):
    return jnp.where(mask, 1.0, 0.0).astype(BF16)


def whole(value):
    return value.astype(F32).astype(BF16)


def dot(left, right):
    return jnp.dot(left, right, preferred_element_type=F32)


def in_three(value):
    high = value.astype(BF16).astype(F32)
    middle = (value - high).astype(BF16).astype(F32)
    low = (value - high - middle).astype(BF16).astype(F32)
    return high, middle, low


def total(value):
    return jnp.sum(jnp.sum(value, axis=0, keepdims=True), axis=1, keepdims=True)


def spreads_of(count, rows_here):
    shape = (count, 2 * count * rows_here)
    message = iota(shape, 1) // rows_here
    return [one_hot(message == iota(shape, 0) * 2 + end) for end in range(2)]


def chosen(slots, spreads, rows, rows_here):
    messages = spreads[0].shape[1]
    row = (iota((1, messages), 1) % rows_here).astype(F32)
    wanted = sum(dot(slot, spread) for slot, spread in zip(slots, spreads)) * rows_here + row
    return one_hot(iota((rows, messages), 0).astype(F32) == wanted)


def slots_of(ends_ref, slot_ref):
    ends = ends_ref[...]
    slot_row = whole(slot_ref[...])
    number = iota((slot_row.shape[1], ends.shape[1]), 0)
    return [
        dot(slot_row, one_hot(number == ends[end : end + 1])).astype(BF16) for end in range(2)
    ]


def select_kernel(groups, ends_ref, slot_ref, wave_ref, out_ref):
    grp = lax.axis_index("grp")
    pairs = ends_ref.shape[1]
    ops = pairs // groups
    sectors, rows_here, width = wave_ref.shape
    rows = sectors * rows_here
    mine = one_hot(iota((pairs, ops), 0) == iota((pairs, ops), 1) * groups + grp)
    slots = [dot(slot, mine).astype(BF16) for slot in slots_of(ends_ref, slot_ref)]
    choose = chosen(slots, spreads_of(ops, rows_here), rows, rows_here)
    wave = wave_ref[...].astype(F32).reshape(rows, width).astype(BF16)
    out_ref[...] = lax.dot_general(
        choose, wave, CONTRACT_ROWS, preferred_element_type=F32
    ).astype(BF16)


def table_kernel(groups, inner, ends_ref, slot_ref, near_ref, every_ref):
    far = lax.axis_index("ops_1") * lax.axis_size("ops_2") + lax.axis_index("ops_2")
    far_count = lax.axis_size("ops_1") * lax.axis_size("ops_2")
    pairs = ends_ref.shape[1]
    ops = pairs // groups
    rows = near_ref.shape[0]
    rows_here = rows // slot_ref.shape[1]
    slots = slots_of(ends_ref, slot_ref)
    spreads = spreads_of(ops, rows_here)
    messages = 2 * ops * rows_here
    for part in range(groups):
        held = slice(part * ops, (part + 1) * ops)
        every_ref[:, part * messages : (part + 1) * messages] = chosen(
            [slot[:, held] for slot in slots], spreads, rows, rows_here
        )
    near_count = pairs // far_count
    member = iota((pairs, near_count), 1)
    pair = (member // inner * far_count + far) * inner + member % inner
    near = one_hot(iota((pairs, near_count), 0) == pair)
    near_ref[...] = chosen(
        [dot(slot, near).astype(BF16) for slot in slots],
        spreads_of(near_count, rows_here),
        rows,
        rows_here,
    )


def pair_products(even, odd, left_ref, right_ref):
    block = left_ref.shape[0]
    tiles, _, width = even.shape
    upper = lax.broadcasted_iota(jnp.int32, even.shape, 1) < 4
    source = jnp.where(upper, even, pltpu.roll(odd, 4, 1)).reshape(block, width).astype(BF16)
    target = jnp.where(upper, pltpu.roll(even, 4, 1), odd).reshape(block, width).astype(BF16)
    left = left_ref[...]
    inner = dot(left, source).astype(BF16)
    flipped = lax.dot_general(left, target, CONTRACT_ROWS, preferred_element_type=F32).astype(BF16)
    right = right_ref[...]
    forward = dot(inner, right).reshape(tiles, 8, width)
    adjoint = lax.dot_general(
        flipped, right, CONTRACT_COLUMNS, preferred_element_type=F32
    ).reshape(tiles, 8, width)
    return (
        jnp.where(upper, adjoint, pltpu.roll(forward, 4, 1)),
        jnp.where(upper, pltpu.roll(adjoint, 4, 1), forward),
    )


def first_pair_kernel(
    fetched_ref, left_ref, right_ref, wave_ref, diag_ref, out_ref
):
    width = right_ref.shape[0]
    tiles = left_ref.shape[0] // 8
    blocks, _, groups, slots, _, share = out_ref.shape
    far = slots - 1
    fetched = fetched_ref[...].astype(F32).reshape(tiles, 2, 8, width)
    even, odd = fetched[:, 0], fetched[:, 1]
    products = pair_products(even, odd, left_ref, right_ref)
    for block in range(blocks):
        for parity, product in enumerate(products):
            for grp in range(groups):
                out_ref[block, parity, grp, :far] = product[
                    block * far : (block + 1) * far, :, grp * share : (grp + 1) * share
                ].astype(BF16)
    wave = wave_ref[...].astype(F32)
    sums = (
        total(jnp.sum(even * products[0] + odd * products[1], axis=0)),
        total(diag_ref[...] * wave * wave),
        total(wave * wave),
    )
    lane = iota((1, share), 1)
    carried = jnp.zeros((1, share), F32)
    for at, term in enumerate(term for value in sums for term in in_three(value)):
        carried = jnp.where(lane == at, term, carried)
    carried = jnp.broadcast_to(carried, (8, share)).astype(BF16)
    for block in range(blocks):
        for parity in range(2):
            for grp in range(groups):
                out_ref[block, parity, grp, far] = carried


def second_pair_kernel(fetched_ref, left_ref, right_ref, out_ref):
    groups, share = fetched_ref.shape[2], fetched_ref.shape[4]
    even, odd = (
        jnp.concatenate(
            [fetched_ref[:, parity, grp].astype(F32) for grp in range(groups)], axis=2
        )
        for parity in range(2)
    )
    products = pair_products(even, odd, left_ref, right_ref)
    for parity, product in enumerate(products):
        for grp in range(groups):
            out_ref[:, parity, grp] = product[:, :, grp * share : (grp + 1) * share].astype(BF16)


def gather_kernel(near_ref, arrived_ref, out_ref):
    members, slots, _, share = arrived_ref.shape
    far = slots - 1
    rows = near_ref.shape[0]
    near = near_ref[...]
    carried = jnp.sum(arrived_ref[:, far].astype(F32), axis=0)
    high, middle, low = in_three(carried)
    place = iota(carried.shape, 0)
    terms = jnp.where(place == 0, high, jnp.where(place == 1, middle, low))
    terms = jnp.where(place < 3, terms, 0.0).astype(BF16)
    for at in range(far):
        arrived = arrived_ref[:, at].reshape(members * 8, share)
        out_ref[at, :rows] = dot(near, arrived).astype(BF16)
        out_ref[at, rows:] = terms


def residual_kernel(groups, arrived_ref, wave_ref, diag_ref, every_ref, residual_ref, base_ref, out_ref):
    rows, share = residual_ref.shape
    arrived = jnp.sum(arrived_ref[...].astype(F32), axis=0)
    carried = jnp.sum(arrived[rows:], axis=0, keepdims=True)
    lane = iota(carried.shape, 1)
    pairs_part = total(jnp.where(lane < 3, carried, 0.0))
    diag_part = total(jnp.where((lane >= 3) & (lane < 6), carried, 0.0)) / groups
    square = total(jnp.where((lane >= 6) & (lane < 9), carried, 0.0)) / groups
    rayleigh = (pairs_part + diag_part) / square
    mine = pl.ds(pl.multiple_of(lax.axis_index("grp") * share, share), share)
    wave = wave_ref[:, mine].astype(F32)
    diag = diag_ref[:, mine]
    residual = diag * wave + arrived[:rows] - rayleigh * wave
    half = residual.astype(BF16)
    residual_ref[...] = residual
    base_ref[...] = diag * half.astype(F32)
    out_ref[...] = lax.dot_general(
        every_ref[...], half, CONTRACT_ROWS, preferred_element_type=F32
    ).astype(BF16)


def final_kernel(every_ref, arrived_ref, base_ref, out_ref):
    out_ref[...] = base_ref[...] + dot(every_ref[...], arrived_ref[...])


def call(kernel, outs, flops, *args, grant=24):
    specs = jax.tree.map(lambda _: VMEM, outs)
    size = sum(arg.size * arg.dtype.itemsize for arg in args)
    return pl.pallas_call(
        kernel,
        out_shape=outs,
        in_specs=[VMEM] * len(args),
        out_specs=specs,
        compiler_params=pltpu.CompilerParams(vmem_limit_bytes=grant << 20),
        cost_estimate=pl.CostEstimate(flops=flops, bytes_accessed=2 * size, transcendentals=0),
    )(*args)


def array(shape, dtype):
    return jax.ShapeDtypeStruct(shape, dtype)


def exchange(value, axes):
    return lax.all_to_all(value, axes, 0, 0, tiled=True)


def body(wave, diag_energy, left_ops, right_ops, pair_sectors, sector_slot):
    ops = lax.axis_size(OPS)
    groups = lax.axis_size("grp")
    far = lax.axis_size(FAR)
    near = lax.axis_size(NEAR)
    blocks = lax.axis_size("ops_0")
    sectors, rows_here, width = wave.shape
    rows = sectors * rows_here
    share = width // groups
    messages = 2 * ops * rows_here
    left, right = left_ops[0], right_ops[0]
    pairs, slots = pair_sectors.T, sector_slot[None]
    outgoing = call(
        functools.partial(select_kernel, groups),
        array((messages, width), BF16),
        200_000_000,
        pairs,
        slots,
        wave,
        grant=60,
    )
    near_choose, every = call(
        functools.partial(table_kernel, groups, near // blocks),
        (
            array((rows, 2 * near * rows_here), BF16),
            array((rows, groups * messages), BF16),
        ),
        2_000_000_000,
        pairs,
        slots,
        grant=60,
    )
    wave = wave.reshape(rows, width)
    diag, near_choose, every = lax.optimization_barrier(
        (diag_energy.reshape(rows, width), near_choose, every)
    )
    fetched = exchange(outgoing.reshape(ops, -1, width), OPS).reshape(messages, width)
    scattered = call(
        first_pair_kernel,
        array((blocks, 2, groups, far + 1, 8, share), BF16),
        1_100_000_000,
        fetched,
        left,
        right,
        wave,
        diag,
    )
    arrived = exchange(scattered.reshape(near, far + 1, 8, share), NEAR)
    partial = call(
        gather_kernel, array((far, rows + 8, share), BF16), 150_000_000, near_choose, arrived
    )
    arrived = exchange(partial, FAR)
    residual, base, outgoing = call(
        functools.partial(residual_kernel, groups),
        (
            array((rows, share), F32),
            array((rows, share), F32),
            array((groups * messages, share), BF16),
        ),
        150_000_000,
        arrived,
        wave,
        diag,
        every,
    )
    fetched = exchange(outgoing.reshape(ops * groups, -1, share), OPS_GRP)
    shape = (ops // 2, 2, groups, 2 * rows_here, share)
    scattered = call(
        second_pair_kernel,
        array(shape, BF16),
        1_100_000_000,
        fetched.reshape(shape),
        left,
        right,
    )
    arrived = exchange(scattered.reshape(ops * groups, -1, share), OPS_GRP)
    sigma_out = call(
        final_kernel,
        array((rows, share), F32),
        150_000_000,
        every,
        arrived.reshape(groups * messages, share),
        base,
    )
    shape = (sectors, rows_here, share)
    return residual.reshape(shape), sigma_out.reshape(shape)


def solution(mesh):
    finer = Mesh(mesh.devices.reshape(4, 4, 4, 2, mesh.shape["grp"]), OPS_GRP)
    return jax.shard_map(
        body,
        mesh=finer,
        in_specs=(
            P(None, OPS, None),
            P(None, OPS, None),
            P(OPS_GRP, None, None),
            P(OPS_GRP, None, None),
            P(),
            P(),
        ),
        out_specs=(P(None, OPS, "grp"), P(None, OPS, "grp")),
        check_vma=False,
    )
```
